32 devices in a mesh: rows: 8 (over z, y), cols: 4 (over x, core).
Axes of the slice: x: 2, y: 2, z: 4, core: 2. Of those that a mesh axis runs over, the one named last changes fastest.
Arguments:
- points: bfloat16 [4096, 256], P(('rows', 'cols')), may hold values from -6 to 6
- start_vectors: float32 [8, 4096], P(None, ('rows', 'cols')), may hold values from -6 to 6
- degree: bfloat16 [4096], P(('rows', 'cols')), may hold values from 0.19921875 to 2
Outputs:
- embedding: float32 [8, 4096], P(None, ('rows', 'cols'))
The draws below stay inside these ranges and needn't reach their ends.
All inputs are finite; a program needn't handle non-finite values.
Results may differ from the reference program's by a relative error of at most 0.0034.
Values may be sent and summed in bfloat16 or wider, within the bound.
A program may use at most 64 MiB of HBM per device.

```python
import math
import jax
import jax.numpy as jnp
from jax import lax

F = 256
K = 8
ITERS = 3
NPTS = 4096


def draw_points(key, part):
    group_size = 16
    clusters = max(NPTS // group_size, 2)
    jitter_sq = 0.5
    centre_sq = math.log(max(NPTS - group_size, 2 * group_size) / (group_size - 1.0)) / 8.0
    key_centre = jax.random.fold_in(key, 11)
    key_label = jax.random.fold_in(key, 12)
    key_jitter = jax.random.fold_in(key, 13)
    labels = jax.random.randint(key_label, (NPTS,), 0, clusters)
    centres = jax.random.normal(key_centre, (clusters, F), jnp.float32) * math.sqrt(centre_sq)
    jitter = jax.random.normal(key_jitter, (NPTS, F), jnp.float32) * math.sqrt(jitter_sq)
    values = centres[labels] + jitter
    return jnp.clip(values, -6.0, 6.0).astype(jnp.bfloat16)


def levels(rng, dims, split, least, top_value):
    gain, own = 1.0, jax.random.fold_in(rng, 6)
    for axis_at, parts in split:
        steps = jnp.exp(jax.random.uniform(jax.random.fold_in(own, axis_at), (parts,), jnp.float32, least / len(split), top_value / len(split)))
        gain = gain * jnp.repeat(steps, dims[axis_at] // parts).reshape([-1 if axis == axis_at else 1 for axis in range(len(dims))])
    return gain


def scatter_about(rng, shape, scale, bound, shards=(), kind=jnp.bfloat16):
    factor_of = levels(rng, shape, shards, -0.22, 0.18) if shards else 1.0
    entries = jax.random.normal(rng, shape, jnp.float32) * scale * factor_of
    return jnp.minimum(jnp.maximum(entries, -bound), bound).astype(kind)


def setup_inputs(seed: int = 0) -> dict:
    streams_of = jax.random.split(jax.random.key(seed), 4)
    return {
        "points": draw_points(jax.random.fold_in(streams_of[3], 71), 0),
        "start_vectors": scatter_about(streams_of[1], (K, NPTS), 1.0, 6.0, ((1, 32),), jnp.float32),
        "degree": jnp.clip(jnp.exp(math.log(2.0) - 2.306499 * jax.random.uniform(streams_of[2], (NPTS,), jnp.float32) ** levels(streams_of[2], (NPTS,), ((0, 32),), -0.2, 0.2)), 0.19921875, 2.0).astype(jnp.bfloat16),
    }


def reference(points, start_vectors, degree):
    npts = points.shape[0]
    sharpness = 4.0 / points.shape[1]
    points_f = points.astype(jnp.float32)
    sqnorm = jnp.sum(points_f * points_f, axis=1)
    block_rows = min(512, npts)
    block_count = npts // block_rows
    all_index = jnp.arange(npts, dtype=jnp.int32)
    degree_f = degree.astype(jnp.float32)

    def apply(vectors):
        sending = vectors.astype(jnp.bfloat16).astype(jnp.float32)

        def one_block(block_index):
            first_row = (block_index * block_rows).astype(jnp.int32)
            row_points = lax.dynamic_slice_in_dim(points_f, first_row, block_rows, 0)
            row_norms = lax.dynamic_slice_in_dim(sqnorm, first_row, block_rows, 0)
            gram = jnp.dot(row_points, points_f.T, precision=lax.Precision.HIGHEST)
            distance = row_norms[:, None] + sqnorm[None, :] - 2.0 * gram
            kernel = jnp.exp(-sharpness * distance)
            row_index = first_row + jnp.arange(block_rows, dtype=jnp.int32)
            kernel = jnp.where(row_index[:, None] == all_index[None, :], jnp.float32(0.0), kernel)
            kernel = lax.optimization_barrier(kernel.astype(jnp.bfloat16)).astype(jnp.float32)
            return jnp.dot(sending, kernel.T, precision=lax.Precision.HIGHEST)

        blocks = lax.map(one_block, jnp.arange(block_count, dtype=jnp.int32))
        return jnp.transpose(blocks, (1, 0, 2)).reshape(vectors.shape[0], npts)

    vectors = start_vectors.astype(jnp.float32)
    for iteration in range(ITERS):
        vectors = apply(vectors) / degree_f[None, :]
    mean_abs = jnp.sum(jnp.abs(vectors), axis=1) / npts
    return vectors / (mean_abs[:, None] + 1e-6)
```

```python
import functools
import math

import jax
import jax.numpy as jnp
from jax import lax
from jax.experimental import pallas as pl
from jax.experimental.pallas import tpu as pltpu
from jax.sharding import PartitionSpec as P

ITERS = 3
MESH = pl.DeviceIdType.MESH
F32, BF16 = jnp.float32, jnp.bfloat16
NT = (((1,), (1,)), ((), ()))
NN = (((1,), (0,)), ((), ()))


def kernel(
    na, nb, nc, x_ref, v_ref, d_ref, o_ref,
    xr, xc, v0, vb, rs, pt, mg, at, hj,
    xr_s, xr_r, xc_s, xc_r, v0_s, v0_r, vb_s, vb_r, rs_s, rs_r, mg_s, mg_r,
):
    span, feats = x_ref.shape
    nq, nd = na // 2, na * nb
    sharp = 4.0 / feats * math.log2(math.e)
    flat = lax.axis_index("rows") * nc + lax.axis_index("cols")
    b, a = flat // na, flat % na
    q, p = a // 2, a % 2

    def device(flat_index):
        return (flat_index // nc, flat_index % nc)

    def member(chip, parity):
        return device(b * na + chip * 2 + parity)

    def line(step):
        return device((b + step + nb) % nb * na + a)

    pending = []

    def send(src, dst, send_sem, recv_sem, target):
        copy = pltpu.make_async_remote_copy(
            src_ref=src, dst_ref=dst, send_sem=send_sem, recv_sem=recv_sem,
            device_id=target, device_id_type=MESH,
        )
        copy.start()
        pending.append(copy)
        return copy

    barrier = pltpu.get_barrier_semaphore()
    for step in range(na):
        if step:
            peer = device(b * na + (a + step) % na)
            pl.semaphore_signal(barrier, inc=1, device_id=peer, device_id_type=MESH)
    for step in range(1, nb):
        pl.semaphore_signal(barrier, inc=1, device_id=line(step), device_id_type=MESH)
    pl.semaphore_wait(barrier, na + nb - 2)

    partner = member(q, 1 - p)
    xr_in, xc_in, v0_in = {}, {}, {}
    for kq in range(1, nq):
        slot = 2 * kq
        xr_in[slot] = send(
            x_ref, xr.at[slot], xr_s.at[slot], xr_r.at[slot], member((q + kq) % nq, p)
        )
    for kb in range(1, nb):
        xc_in[kb] = send(x_ref, xc.at[kb], xc_s.at[kb], xc_r.at[kb], line(kb))
    for kb in range(1, nb):
        v0_in[kb] = send(v_ref, v0.at[kb], v0_s.at[kb], v0_r.at[kb], line(kb))
    xr_in[1] = send(x_ref, xr.at[1], xr_s.at[1], xr_r.at[1], partner)

    def squares(x):
        xf = x.astype(F32)
        sq = xf * xf
        high = sq.astype(BF16)
        return high, (sq - high.astype(F32)).astype(BF16)

    wide = jnp.ones((feats, 128), BF16)
    thin = jnp.ones((8, feats), BF16)

    def dot(l, r, dims):
        return lax.dot_general(l, r, dims, preferred_element_type=F32)

    def store_norm(kb, x):
        high, low = squares(x)
        hj[kb] = sharp * (dot(high, wide, NN) + dot(low, wide, NN))

    def row_norm(x):
        high, low = squares(x)
        return (sharp * (dot(thin, high, NT) + dot(thin, low, NT)))[0:1, :]

    def unit(kb, kq, xj, xi, hi, diagonal=False):
        g = dot(xj, xi, NT)
        hcol = hj[kb]
        for half in range(2):
            lanes = slice(half * span, (half + 1) * span)
            e = jnp.exp2((2.0 * sharp) * g[:, lanes] - (hcol + hi[:, lanes]))
            if diagonal and half == 0:
                rows = lax.broadcasted_iota(jnp.int32, (span, span), 0)
                cols = lax.broadcasted_iota(jnp.int32, (span, span), 1)
                e = jnp.where(rows == cols, 0.0, e)
            at[kb, :, (2 * kq + half) * span:(2 * kq + half + 1) * span] = e.astype(BF16)

    def others(body):
        if nb <= 4:
            for kb in range(1, nb):
                body(kb)
        else:
            def looped(kb, carry):
                body(kb)
                return carry
            lax.fori_loop(1, nb, looped, 0)

    own = x_ref[...]
    store_norm(0, own)
    xr_in[1].wait_recv()
    xi = jnp.concatenate([own, xr[1]], axis=0)
    hi0 = row_norm(xi)
    unit(0, 0, own, xi, hi0, diagonal=True)

    for kq in range(1, nq):
        slot = 2 * kq
        xr_in[slot].wait_recv()
        xr_in[slot + 1] = send(
            xr.at[slot], xr.at[slot + 1], xr_s.at[slot + 1], xr_r.at[slot + 1], partner
        )
    for kb in range(1, nb):
        xc_in[kb].wait_recv()

    def first(kb):
        xj = xc[kb]
        store_norm(kb, xj)
        unit(kb, 0, xj, xi, hi0)

    others(first)
    for kq in range(1, nq):
        xr_in[2 * kq + 1].wait_recv()
        pair = jnp.concatenate([xr[2 * kq], xr[2 * kq + 1]], axis=0)
        hi = row_norm(pair)
        unit(0, kq, own, pair, hi)

        def more(kb, kq=kq, pair=pair, hi=hi):
            unit(kb, kq, xc[kb], pair, hi)

        others(more)

    for kb in range(1, nb):
        v0_in[kb].wait_recv()
    v_parts = [v_ref[...].astype(BF16)] + [v0[kb].astype(BF16) for kb in range(1, nb)]
    inv = d_ref[...].astype(F32)

    for it in range(ITERS):
        product = jnp.zeros((v_ref.shape[0], na * span), F32)
        for kb in range(nb):
            product = product + dot(v_parts[kb], at[kb], NN)
        rs_in = {}
        for slot in range(1, na):
            pt[it, slot] = product[:, slot * span:(slot + 1) * span]
        for slot in range(1, na):
            kq, kp = slot // 2, slot % 2
            parity = p if kp == 0 else 1 - p
            rs_in[slot] = send(
                pt.at[it, slot], rs.at[it, slot], rs_s.at[it, slot], rs_r.at[it, slot],
                member((q - kq + nq) % nq, parity),
            )
        total = product[:, :span]
        for slot in range(1, na):
            rs_in[slot].wait_recv()
            total = total + rs[it, slot]
        mine = total / inv
        if it < ITERS - 1:
            sending = mine.astype(BF16)
            vb[it, 0] = sending
            vb_in = {}
            for kb in range(1, nb):
                vb_in[kb] = send(
                    vb.at[it, 0], vb.at[it, kb], vb_s.at[it, kb], vb_r.at[it, kb], line(kb)
                )
            v_parts = [sending]
            for kb in range(1, nb):
                vb_in[kb].wait_recv()
                v_parts.append(vb[it, kb])

    nk = v_ref.shape[0]
    sums = jnp.sum(jnp.abs(mine), axis=1, keepdims=True)
    eye = lax.broadcasted_iota(jnp.int32, (nk, 128), 0) == lax.broadcasted_iota(
        jnp.int32, (nk, 128), 1
    )
    mg[0] = jnp.sum(jnp.where(eye, sums, 0.0), axis=0, keepdims=True)

    def spread(step):
        return pltpu.make_async_remote_copy(
            src_ref=mg.at[0], dst_ref=mg.at[step], send_sem=mg_s.at[step],
            recv_sem=mg_r.at[step], device_id=device((flat + step) % nd),
            device_id_type=MESH,
        )

    def start_one(step, carry):
        spread(step).start()
        return carry

    def wait_one(step, carry):
        spread(step).wait_recv()
        return carry

    def done_one(step, carry):
        spread(step).wait_send()
        return carry

    lax.fori_loop(1, nd, start_one, 0)
    for copy in pending:
        copy.wait_send()
    lax.fori_loop(1, nd, wait_one, 0)
    every = jnp.sum(mg[...], axis=0)
    mean = jnp.sum(jnp.where(eye, every, 0.0), axis=1, keepdims=True) / (span * nd)
    o_ref[...] = mine / (mean + 1e-06)
    lax.fori_loop(1, nd, done_one, 0)


def solution(mesh):
    nr, nc = mesh.shape["rows"], mesh.shape["cols"]
    low = 1
    while low * nc < nr // low:
        low *= 2
    na, nb = low * nc, nr // low

    def body(points, start_vectors, degree):
        span, feats = points.shape
        nk = start_vectors.shape[0]
        dma = pltpu.SemaphoreType.DMA
        return pl.pallas_call(
            functools.partial(kernel, na, nb, nc),
            out_shape=jax.ShapeDtypeStruct((nk, span), F32),
            in_specs=[pl.BlockSpec(memory_space=pltpu.VMEM)] * 3,
            out_specs=pl.BlockSpec(memory_space=pltpu.VMEM),
            scratch_shapes=[
                pltpu.VMEM((na, span, feats), BF16),
                pltpu.VMEM((nb, span, feats), BF16),
                pltpu.VMEM((nb, nk, span), F32),
                pltpu.VMEM((ITERS - 1, nb, nk, span), BF16),
                pltpu.VMEM((ITERS, na, nk, span), F32),
                pltpu.VMEM((ITERS, na, nk, span), F32),
                pltpu.VMEM((na * nb, 1, 128), F32),
                pltpu.VMEM((nb, span, na * span), BF16),
                pltpu.VMEM((nb, span, 128), F32),
                dma((na,)), dma((na,)), dma((nb,)), dma((nb,)), dma((nb,)), dma((nb,)),
                dma((ITERS - 1, nb)), dma((ITERS - 1, nb)),
                dma((ITERS, na)), dma((ITERS, na)),
                dma((na * nb,)), dma((na * nb,)),
            ],
            compiler_params=pltpu.CompilerParams(collective_id=0, has_side_effects=True),
        )(points, start_vectors, degree.reshape(1, span))

    return jax.shard_map(
        body,
        mesh=mesh,
        in_specs=(P(("rows", "cols"), None), P(None, ("rows", "cols")), P(("rows", "cols"))),
        out_specs=P(None, ("rows", "cols")),
        check_vma=False,
    )
```

```python
import functools
import math

import jax
import jax.numpy as jnp
from jax import lax
from jax.experimental import pallas as pl
from jax.experimental.pallas import tpu as pltpu
from jax.sharding import PartitionSpec as P

ITERS = 3
MESH = pl.DeviceIdType.MESH
F32, BF16 = jnp.float32, jnp.bfloat16
NT = (((1,), (1,)), ((), ()))
NN = (((1,), (0,)), ((), ()))


def kernel(
    na, nb, nc, x_hbm, v_hbm, d_hbm, o_ref,
    xr, xc, v0, db, da, zb, ab, mg, at, hj, d_ref, in_s,
    xr_s, xr_r, xc_s, xc_r, v0_s, v0_r, db_s, db_r, da_s, da_r,
    zb_s, zb_r, ab_s, ab_r, mg_s, mg_r,
):
    span, feats = x_hbm.shape
    nk = v_hbm.shape[0]
    nq, nd = na // 2, na * nb
    x_ref, v_ref = xr.at[0], v0.at[0]
    sharp = 4.0 / feats * math.log2(math.e)
    flat = lax.axis_index("rows") * nc + lax.axis_index("cols")
    b, a = flat // na, flat % na
    q, p = a // 2, a % 2

    def device(flat_index):
        return (flat_index // nc, flat_index % nc)

    def member(chip, parity):
        return device(b * na + chip * 2 + parity)

    def line(step):
        return device((b + step + nb) % nb * na + a)

    pending = []

    def send(src, dst, send_sem, recv_sem, target):
        copy = pltpu.make_async_remote_copy(
            src_ref=src, dst_ref=dst, send_sem=send_sem, recv_sem=recv_sem,
            device_id=target, device_id_type=MESH,
        )
        copy.start()
        pending.append(copy)
        return copy

    loads = [
        pltpu.make_async_copy(src, dst, in_s.at[i])
        for i, (src, dst) in enumerate([(x_hbm, x_ref), (v_hbm, v_ref), (d_hbm, d_ref)])
    ]
    for load in loads:
        load.start()

    barrier = pltpu.get_barrier_semaphore()
    for step in range(na):
        if step:
            peer = device(b * na + (a + step) % na)
            pl.semaphore_signal(barrier, inc=1, device_id=peer, device_id_type=MESH)
    for step in range(1, nb):
        pl.semaphore_signal(barrier, inc=1, device_id=line(step), device_id_type=MESH)
    loads[2].wait()
    degree = d_ref[...].astype(F32)
    db[0] = degree
    da[0] = degree
    loads[0].wait()
    loads[1].wait()
    pl.semaphore_wait(barrier, na + nb - 2)

    partner = member(q, 1 - p)

    def slot_member(slot):
        kq, kp = slot // 2, slot % 2
        return member((q + kq) % nq, p if kp == 0 else 1 - p)

    relay = nb == 4
    x_in, xc_in, v_in, db_in, da_in = {}, {}, {}, {}, {}

    def to_line(step):
        return pltpu.make_async_remote_copy(
            src_ref=x_ref, dst_ref=xc.at[step], send_sem=xc_s.at[step],
            recv_sem=xc_r.at[step], device_id=line(step), device_id_type=MESH,
        )

    order = [3, 1] if relay else list(range(1, nb))
    if relay:
        @pl.when(b % 3 == 0)
        def _():
            to_line(2).start()
    for kb in order:
        xc_in[kb] = send(x_ref, xc.at[kb], xc_s.at[kb], xc_r.at[kb], line(kb))
    for kq in range(1, nq):
        slot = 2 * kq
        x_in[slot] = send(x_ref, xr.at[slot], xr_s.at[slot], xr_r.at[slot], slot_member(slot))
    x_in[1] = send(x_ref, xr.at[1], xr_s.at[1], xr_r.at[1], partner)
    for kq in range(1, nq):
        slot = 2 * kq
        v_in[slot] = send(v_ref, v0.at[slot], v0_s.at[slot], v0_r.at[slot], slot_member(slot))
    v_in[1] = send(v_ref, v0.at[1], v0_s.at[1], v0_r.at[1], partner)
    for kb in range(1, nb):
        db_in[kb] = send(db.at[0], db.at[kb], db_s.at[kb], db_r.at[kb], line(kb))
    for slot in range(1, na):
        da_in[slot] = send(da.at[0], da.at[slot], da_s.at[slot], da_r.at[slot], slot_member(slot))

    def squares(x):
        xf = x.astype(F32)
        sq = xf * xf
        high = sq.astype(BF16)
        return high, (sq - high.astype(F32)).astype(BF16)

    wide = jnp.ones((feats, 128), BF16)
    thin = jnp.ones((8, feats), BF16)

    def dot(l, r, dims):
        return lax.dot_general(l, r, dims, preferred_element_type=F32)

    def store_norm(kb, x):
        high, low = squares(x)
        hj[kb] = sharp * (dot(high, wide, NN) + dot(low, wide, NN))

    def row_norm(x):
        high, low = squares(x)
        return (sharp * (dot(thin, high, NT) + dot(thin, low, NT)))[0:1, :]

    def unit(kb, kq, xj, xi, hi, diagonal=False):
        g = dot(xj, xi, NT)
        hcol = hj[kb]
        for half in range(2):
            lanes = slice(half * span, (half + 1) * span)
            e = jnp.exp2((2.0 * sharp) * g[:, lanes] - (hcol + hi[:, lanes]))
            if diagonal and half == 0:
                rows = lax.broadcasted_iota(jnp.int32, (span, span), 0)
                cols = lax.broadcasted_iota(jnp.int32, (span, span), 1)
                e = jnp.where(rows == cols, 0.0, e)
            at[kb, :, (2 * kq + half) * span:(2 * kq + half + 1) * span] = e.astype(BF16)

    def others(body):
        if nb <= 4:
            for kb in range(1, nb):
                body(kb)
        else:
            def looped(kb, carry):
                body(kb)
                return carry
            lax.fori_loop(1, nb, looped, 0)

    own = x_ref[...]
    store_norm(0, own)
    x_in[1].wait_recv()
    xi = jnp.concatenate([own, xr[1]], axis=0)
    hi0 = row_norm(xi)
    unit(0, 0, own, xi, hi0, diagonal=True)

    def pass_on(slot):
        x_in[slot].wait_recv()
        x_in[slot + 1] = send(
            xr.at[slot], xr.at[slot + 1], xr_s.at[slot + 1], xr_r.at[slot + 1], partner
        )

    def first(kb):
        xj = xc[kb]
        store_norm(kb, xj)
        unit(kb, 0, xj, xi, hi0)

    if relay:
        xc_in[1].wait_recv()
        xc_in[3].wait_recv()

        @pl.when(b % 3 != 0)
        def _():
            pltpu.make_async_remote_copy(
                src_ref=xc.at[(5 - 2 * b) % 4], dst_ref=xc.at[2], send_sem=xc_s.at[2],
                recv_sem=xc_r.at[2], device_id=line(2 * b - 3), device_id_type=MESH,
            ).start()
    for kq in range(1, nq):
        pass_on(2 * kq)
    for kq in range(1, nq):
        slot = 2 * kq
        v_in[slot].wait_recv()
        v_in[slot + 1] = send(
            v0.at[slot], v0.at[slot + 1], v0_s.at[slot + 1], v0_r.at[slot + 1], partner
        )
    if relay:
        first(1)
        first(3)
    his, pairs = [hi0], [xi]
    for kq in range(1, nq):
        x_in[2 * kq + 1].wait_recv()
        pairs.append(jnp.concatenate([xr[2 * kq], xr[2 * kq + 1]], axis=0))
        his.append(row_norm(pairs[kq]))
        unit(0, kq, own, pairs[kq], his[kq])
        if relay:
            unit(1, kq, xc[1], pairs[kq], his[kq])
            unit(3, kq, xc[3], pairs[kq], his[kq])
    if relay:
        to_line(2).wait_recv()
    else:
        for kb in range(1, nb):
            xc_in[kb].wait_recv()

    def rest(kb):
        first(kb)
        for kq in range(1, nq):
            unit(kb, kq, xc[kb], pairs[kq], his[kq])

    if relay:
        rest(2)
    else:
        others(rest)

    for slot in range(1, na):
        if slot % 2:
            v_in[slot].wait_recv()
        da_in[slot].wait_recv()
    for kb in range(1, nb):
        db_in[kb].wait_recv()
    col_degree = [db[kb] for kb in range(nb)]
    row_degree = [da[slot] for slot in range(na)]

    def to_columns(turn, row_vectors):
        wide_rows = jnp.concatenate(row_vectors, axis=1)
        part = [dot(wide_rows, at[kb], NT) for kb in range(nb)]
        for kb in range(nb):
            zb[turn, 0, :, kb * span:(kb + 1) * span] = part[kb]
        arriving = {
            kb: send(
                zb.at[turn, 0], zb.at[turn, kb], zb_s.at[turn, kb], zb_r.at[turn, kb], line(kb)
            )
            for kb in list(range(2, nb)) + [1]
        }
        for step in range(1, nb):
            arriving[step].wait_recv()
            for kb in range(nb):
                there = (kb - step) % nb
                part[kb] = part[kb] + zb[turn, step, :, there * span:(there + 1) * span]
        return [part[kb] / col_degree[kb] for kb in range(nb)]

    def to_rows(col_vectors):
        part = dot(col_vectors[0], at[0], NN)
        for kb in range(1, nb):
            part = part + dot(col_vectors[kb], at[kb], NN)
        ab[0] = part
        arriving = {
            slot: send(ab.at[0], ab.at[slot], ab_s.at[slot], ab_r.at[slot], slot_member(slot))
            for slot in list(range(2, na)) + [1]
        }
        part = [part[:, slot * span:(slot + 1) * span] for slot in range(na)]
        for step in [1] + list(range(2, na)):
            arriving[step].wait_recv()
            for slot in range(na):
                there = (slot // 2 - step // 2) % nq * 2 + (slot % 2 + step % 2) % 2
                part[slot] = part[slot] + ab[step, :, there * span:(there + 1) * span]
        return [part[slot] / row_degree[slot] for slot in range(na)]

    def rounded(vectors):
        return [piece.astype(BF16) for piece in vectors]

    vectors, on_rows, turn = [v0[slot] for slot in range(na)], True, 0
    for it in range(ITERS):
        if on_rows:
            vectors = to_columns(turn, rounded(vectors))
            turn += 1
        else:
            vectors = to_rows(rounded(vectors))
        on_rows = not on_rows
    mine = vectors[0]

    held = jnp.abs(mine)
    for kb in range(1, nb):
        held = held + jnp.abs(vectors[kb])
    sums = jnp.sum(held, axis=1, keepdims=True)
    eye = lax.broadcasted_iota(jnp.int32, (nk, 128), 0) == lax.broadcasted_iota(
        jnp.int32, (nk, 128), 1
    )
    mg[0] = jnp.sum(jnp.where(eye, sums, 0.0), axis=0, keepdims=True)

    mg_in = {
        slot: send(mg.at[0], mg.at[slot], mg_s.at[slot], mg_r.at[slot], slot_member(slot))
        for slot in list(range(2, na)) + [1]
    }
    for copy in pending[:-(na - 1)]:
        copy.wait_send()
    if relay:
        to_line(2).wait_send()
    for slot in range(1, na):
        mg_in[slot].wait_recv()
    every = jnp.sum(mg[...], axis=0)
    mean = jnp.sum(jnp.where(eye, every, 0.0), axis=1, keepdims=True) / (span * nd)
    o_ref[...] = mine / (mean + 1e-06)
    for slot in range(1, na):
        mg_in[slot].wait_send()


def solution(mesh):
    nr, nc = mesh.shape["rows"], mesh.shape["cols"]
    low = 1
    while low * nc < nr // low:
        low *= 2
    na, nb = low * nc, nr // low

    def body(points, start_vectors, degree):
        span, feats = points.shape
        nk = start_vectors.shape[0]
        dma = pltpu.SemaphoreType.DMA
        turns = (ITERS + 1) // 2
        return pl.pallas_call(
            functools.partial(kernel, na, nb, nc),
            out_shape=jax.ShapeDtypeStruct((nk, span), F32),
            in_specs=[pl.BlockSpec(memory_space=pl.ANY)] * 3,
            out_specs=pl.BlockSpec(memory_space=pltpu.VMEM),
            scratch_shapes=[
                pltpu.VMEM((na, span, feats), BF16),
                pltpu.VMEM((nb, span, feats), BF16),
                pltpu.VMEM((na, nk, span), F32),
                pltpu.VMEM((nb, 1, span), F32),
                pltpu.VMEM((na, 1, span), F32),
                pltpu.VMEM((turns, nb, nk, nb * span), F32),
                pltpu.VMEM((na, nk, na * span), F32),
                pltpu.VMEM((na, 1, 128), F32),
                pltpu.VMEM((nb, span, na * span), BF16),
                pltpu.VMEM((nb, span, 128), F32),
                pltpu.VMEM((1, span), BF16),
                dma((3,)),
                dma((na,)), dma((na,)), dma((nb,)), dma((nb,)), dma((na,)), dma((na,)),
                dma((nb,)), dma((nb,)), dma((na,)), dma((na,)),
                dma((turns, nb)), dma((turns, nb)), dma((na,)), dma((na,)),
                dma((na,)), dma((na,)),
            ],
            compiler_params=pltpu.CompilerParams(collective_id=0, has_side_effects=True),
        )(points, start_vectors, degree.reshape(1, span))

    return jax.shard_map(
        body,
        mesh=mesh,
        in_specs=(P(("rows", "cols"), None), P(None, ("rows", "cols")), P(("rows", "cols"))),
        out_specs=P(None, ("rows", "cols")),
        check_vma=False,
    )
```

```python
import functools
import math

import jax
import jax.numpy as jnp
from jax import lax
from jax.experimental import pallas as pl
from jax.experimental.pallas import tpu as pltpu
from jax.sharding import PartitionSpec as P

ITERS = 3
MESH = pl.DeviceIdType.MESH
F32, BF16 = jnp.float32, jnp.bfloat16
NT = (((1,), (1,)), ((), ()))
NN = (((1,), (0,)), ((), ()))


def kernel(
    na, nb, nc, x_hbm, v_hbm, d_hbm, o_ref,
    xr, xc, v0, db, da, zb, ab, mg, at, hj, d_ref, in_s,
    xr_s, xr_r, xc_s, xc_r, v0_s, v0_r, db_s, db_r, da_s, da_r,
    zb_s, zb_r, ab_s, ab_r, mg_s, mg_r,
):
    span, feats = x_hbm.shape
    nk = v_hbm.shape[0]
    nq, nd = na // 2, na * nb
    x_ref, v_ref = xr.at[0], v0.at[0]
    sharp = 4.0 / feats * math.log2(math.e)
    flat = lax.axis_index("rows") * nc + lax.axis_index("cols")
    b, a = flat // na, flat % na
    q, p = a // 2, a % 2

    def device(flat_index):
        return (flat_index // nc, flat_index % nc)

    def member(chip, parity):
        return device(b * na + chip * 2 + parity)

    def line(step):
        return device((b + step + nb) % nb * na + a)

    pending = []

    def send(src, dst, send_sem, recv_sem, target):
        copy = pltpu.make_async_remote_copy(
            src_ref=src, dst_ref=dst, send_sem=send_sem, recv_sem=recv_sem,
            device_id=target, device_id_type=MESH,
        )
        copy.start()
        pending.append(copy)
        return copy

    loads = [
        pltpu.make_async_copy(src, dst, in_s.at[i])
        for i, (src, dst) in enumerate([(x_hbm, x_ref), (v_hbm, v_ref), (d_hbm, d_ref)])
    ]
    for load in loads:
        load.start()

    barrier = pltpu.get_barrier_semaphore()
    for step in range(na):
        if step:
            peer = device(b * na + (a + step) % na)
            pl.semaphore_signal(barrier, inc=1, device_id=peer, device_id_type=MESH)
    for step in range(1, nb):
        pl.semaphore_signal(barrier, inc=1, device_id=line(step), device_id_type=MESH)
    loads[2].wait()
    degree = d_ref[...].astype(F32)
    db[0] = degree
    da[0] = degree
    loads[0].wait()
    loads[1].wait()
    pl.semaphore_wait(barrier, na + nb - 2)

    partner = member(q, 1 - p)

    def slot_member(slot):
        kq, kp = slot // 2, slot % 2
        return member((q + kq) % nq, p if kp == 0 else 1 - p)

    x_in, xc_in, v_in, db_in, da_in = {}, {}, {}, {}, {}

    for kb in range(1, nb):
        xc_in[kb] = send(x_ref, xc.at[kb], xc_s.at[kb], xc_r.at[kb], line(kb))
    for kq in range(1, nq):
        slot = 2 * kq
        x_in[slot] = send(x_ref, xr.at[slot], xr_s.at[slot], xr_r.at[slot], slot_member(slot))
    x_in[1] = send(x_ref, xr.at[1], xr_s.at[1], xr_r.at[1], partner)
    for kq in range(1, nq):
        slot = 2 * kq
        v_in[slot] = send(v_ref, v0.at[slot], v0_s.at[slot], v0_r.at[slot], slot_member(slot))
    v_in[1] = send(v_ref, v0.at[1], v0_s.at[1], v0_r.at[1], partner)
    for kb in range(1, nb):
        db_in[kb] = send(db.at[0], db.at[kb], db_s.at[kb], db_r.at[kb], line(kb))
    for slot in range(1, na):
        da_in[slot] = send(da.at[0], da.at[slot], da_s.at[slot], da_r.at[slot], slot_member(slot))

    def squares(x):
        xf = x.astype(F32)
        sq = xf * xf
        high = sq.astype(BF16)
        return high, (sq - high.astype(F32)).astype(BF16)

    wide = jnp.ones((feats, 128), BF16)
    thin = jnp.ones((8, feats), BF16)

    def dot(l, r, dims):
        return lax.dot_general(l, r, dims, preferred_element_type=F32)

    def store_norm(kb, x):
        high, low = squares(x)
        hj[kb] = sharp * (dot(high, wide, NN) + dot(low, wide, NN))

    def row_norm(x):
        high, low = squares(x)
        return (sharp * (dot(thin, high, NT) + dot(thin, low, NT)))[0:1, :]

    def unit(kb, kq, xj, xi, hi, diagonal=False):
        g = dot(xj, xi, NT)
        hcol = hj[kb]
        for half in range(2):
            lanes = slice(half * span, (half + 1) * span)
            e = jnp.exp2((2.0 * sharp) * g[:, lanes] - (hcol + hi[:, lanes]))
            if diagonal and half == 0:
                rows = lax.broadcasted_iota(jnp.int32, (span, span), 0)
                cols = lax.broadcasted_iota(jnp.int32, (span, span), 1)
                e = jnp.where(rows == cols, 0.0, e)
            at[kb, :, (2 * kq + half) * span:(2 * kq + half + 1) * span] = e.astype(BF16)

    def others(body):
        if nb <= 4:
            for kb in range(1, nb):
                body(kb)
        else:
            def looped(kb, carry):
                body(kb)
                return carry
            lax.fori_loop(1, nb, looped, 0)

    own = x_ref[...]
    store_norm(0, own)
    x_in[1].wait_recv()
    xi = jnp.concatenate([own, xr[1]], axis=0)
    hi0 = row_norm(xi)
    unit(0, 0, own, xi, hi0, diagonal=True)

    def pass_on(slot):
        x_in[slot].wait_recv()
        x_in[slot + 1] = send(
            xr.at[slot], xr.at[slot + 1], xr_s.at[slot + 1], xr_r.at[slot + 1], partner
        )

    def first(kb):
        xj = xc[kb]
        store_norm(kb, xj)
        unit(kb, 0, xj, xi, hi0)

    for kq in range(1, nq):
        pass_on(2 * kq)
    for kq in range(1, nq):
        slot = 2 * kq
        v_in[slot].wait_recv()
        v_in[slot + 1] = send(
            v0.at[slot], v0.at[slot + 1], v0_s.at[slot + 1], v0_r.at[slot + 1], partner
        )
    for kb in range(1, nb):
        xc_in[kb].wait_recv()
    others(first)
    his, pairs = [hi0], [xi]
    for kq in range(1, nq):
        x_in[2 * kq + 1].wait_recv()
        pairs.append(jnp.concatenate([xr[2 * kq], xr[2 * kq + 1]], axis=0))
        his.append(row_norm(pairs[kq]))
        unit(0, kq, own, pairs[kq], his[kq])

        def more(kb, kq=kq):
            unit(kb, kq, xc[kb], pairs[kq], his[kq])

        others(more)

    for slot in range(1, na):
        if slot % 2:
            v_in[slot].wait_recv()
        da_in[slot].wait_recv()
    for kb in range(1, nb):
        db_in[kb].wait_recv()
    col_degree = [db[kb] for kb in range(nb)]
    row_degree = [da[slot] for slot in range(na)]

    def to_columns(turn, row_vectors):
        wide_rows = jnp.concatenate(row_vectors, axis=1)
        part = [dot(wide_rows, at[kb], NT) for kb in range(nb)]
        for kb in range(nb):
            zb[turn, 0, :, kb * span:(kb + 1) * span] = part[kb]
        arriving = {
            kb: send(
                zb.at[turn, 0], zb.at[turn, kb], zb_s.at[turn, kb], zb_r.at[turn, kb], line(kb)
            )
            for kb in list(range(2, nb)) + [1]
        }
        for step in range(1, nb):
            arriving[step].wait_recv()
            for kb in range(nb):
                there = (kb - step) % nb
                part[kb] = part[kb] + zb[turn, step, :, there * span:(there + 1) * span]
        return [part[kb] / col_degree[kb] for kb in range(nb)]

    def to_rows(col_vectors):
        part = dot(col_vectors[0], at[0], NN)
        for kb in range(1, nb):
            part = part + dot(col_vectors[kb], at[kb], NN)
        ab[0] = part
        arriving = {
            slot: send(ab.at[0], ab.at[slot], ab_s.at[slot], ab_r.at[slot], slot_member(slot))
            for slot in list(range(2, na)) + [1]
        }
        part = [part[:, slot * span:(slot + 1) * span] for slot in range(na)]
        for step in [1] + list(range(2, na)):
            arriving[step].wait_recv()
            for slot in range(na):
                there = (slot // 2 - step // 2) % nq * 2 + (slot % 2 + step % 2) % 2
                part[slot] = part[slot] + ab[step, :, there * span:(there + 1) * span]
        return [part[slot] / row_degree[slot] for slot in range(na)]

    def rounded(vectors):
        return [piece.astype(BF16) for piece in vectors]

    vectors, on_rows, turn = [v0[slot] for slot in range(na)], True, 0
    for it in range(ITERS):
        if on_rows:
            vectors = to_columns(turn, rounded(vectors))
            turn += 1
        else:
            vectors = to_rows(rounded(vectors))
        on_rows = not on_rows
    mine = vectors[0]

    held = jnp.abs(mine)
    for kb in range(1, nb):
        held = held + jnp.abs(vectors[kb])
    sums = jnp.sum(held, axis=1, keepdims=True)
    eye = lax.broadcasted_iota(jnp.int32, (nk, 128), 0) == lax.broadcasted_iota(
        jnp.int32, (nk, 128), 1
    )
    mg[0] = jnp.sum(jnp.where(eye, sums, 0.0), axis=0, keepdims=True)

    mg_in = {
        slot: send(mg.at[0], mg.at[slot], mg_s.at[slot], mg_r.at[slot], slot_member(slot))
        for slot in list(range(2, na)) + [1]
    }
    for copy in pending[:-(na - 1)]:
        copy.wait_send()
    for slot in range(1, na):
        mg_in[slot].wait_recv()
    every = jnp.sum(mg[...], axis=0)
    mean = jnp.sum(jnp.where(eye, every, 0.0), axis=1, keepdims=True) / (span * nd)
    o_ref[...] = mine / (mean + 1e-06)
    for slot in range(1, na):
        mg_in[slot].wait_send()


def solution(mesh):
    nr, nc = mesh.shape["rows"], mesh.shape["cols"]
    low = 1
    while low * nc < nr // low:
        low *= 2
    na, nb = low * nc, nr // low

    def body(points, start_vectors, degree):
        span, feats = points.shape
        nk = start_vectors.shape[0]
        dma = pltpu.SemaphoreType.DMA
        turns = (ITERS + 1) // 2
        return pl.pallas_call(
            functools.partial(kernel, na, nb, nc),
            out_shape=pltpu.VMEM((nk, span), F32),
            in_specs=[pl.BlockSpec(memory_space=pl.ANY)] * 3,
            out_specs=pl.BlockSpec(memory_space=pltpu.VMEM),
            scratch_shapes=[
                pltpu.VMEM((na, span, feats), BF16),
                pltpu.VMEM((nb, span, feats), BF16),
                pltpu.VMEM((na, nk, span), F32),
                pltpu.VMEM((nb, 1, span), F32),
                pltpu.VMEM((na, 1, span), F32),
                pltpu.VMEM((turns, nb, nk, nb * span), F32),
                pltpu.VMEM((na, nk, na * span), F32),
                pltpu.VMEM((na, 1, 128), F32),
                pltpu.VMEM((nb, span, na * span), BF16),
                pltpu.VMEM((nb, span, 128), F32),
                pltpu.VMEM((1, span), BF16),
                dma((3,)),
                dma((na,)), dma((na,)), dma((nb,)), dma((nb,)), dma((na,)), dma((na,)),
                dma((nb,)), dma((nb,)), dma((na,)), dma((na,)),
                dma((turns, nb)), dma((turns, nb)), dma((na,)), dma((na,)),
                dma((na,)), dma((na,)),
            ],
            compiler_params=pltpu.CompilerParams(collective_id=0, has_side_effects=True),
        )(points, start_vectors, degree.reshape(1, span))

    return jax.shard_map(
        body,
        mesh=mesh,
        in_specs=(P(("rows", "cols"), None), P(None, ("rows", "cols")), P(("rows", "cols"))),
        out_specs=P(None, ("rows", "cols")),
        check_vma=False,
    )
```

```python
import functools
import math

import jax
import jax.numpy as jnp
from jax import lax
from jax.experimental import pallas as pl
from jax.experimental.pallas import tpu as pltpu
from jax.sharding import PartitionSpec as P

ITERS = 3
MESH = pl.DeviceIdType.MESH
F32, BF16 = jnp.float32, jnp.bfloat16
NT = (((1,), (1,)), ((), ()))
NN = (((1,), (0,)), ((), ()))


def kernel(
    na, nb, nc, x_hbm, v_hbm, d_hbm, o_ref,
    xr, xc, v0, db, da, zb, ab, mg, at, hj, d_ref, in_s,
    xr_s, xr_r, xc_s, xc_r, v0_s, v0_r, db_s, db_r, da_s, da_r,
    zb_s, zb_r, ab_s, ab_r, mg_s, mg_r,
):
    span, feats = x_hbm.shape
    nk = v_hbm.shape[0]
    nq, nd = na // 2, na * nb
    x_ref, v_ref = xr.at[0], v0.at[0]
    sharp = 4.0 / feats * math.log2(math.e)
    flat = lax.axis_index("rows") * nc + lax.axis_index("cols")
    b, a = flat // na, flat % na
    q, p = a // 2, a % 2

    def device(flat_index):
        return (flat_index // nc, flat_index % nc)

    def member(chip, parity):
        return device(b * na + chip * 2 + parity)

    def line(step):
        return device((b + step + nb) % nb * na + a)

    pending = []

    def send(src, dst, send_sem, recv_sem, target):
        copy = pltpu.make_async_remote_copy(
            src_ref=src, dst_ref=dst, send_sem=send_sem, recv_sem=recv_sem,
            device_id=target, device_id_type=MESH,
        )
        copy.start()
        pending.append(copy)
        return copy

    loads = [
        pltpu.make_async_copy(src, dst, in_s.at[i])
        for i, (src, dst) in enumerate([(x_hbm, x_ref), (v_hbm, v_ref), (d_hbm, d_ref)])
    ]
    for load in loads:
        load.start()

    barrier = pltpu.get_barrier_semaphore()
    for step in range(na):
        if step:
            peer = device(b * na + (a + step) % na)
            pl.semaphore_signal(barrier, inc=1, device_id=peer, device_id_type=MESH)
    for step in range(1, nb):
        pl.semaphore_signal(barrier, inc=1, device_id=line(step), device_id_type=MESH)
    loads[2].wait()
    degree = d_ref[...].astype(F32)
    db[0] = degree
    da[0] = degree
    loads[0].wait()
    loads[1].wait()
    pl.semaphore_wait(barrier, na + nb - 2)

    partner = member(q, 1 - p)

    def slot_member(slot):
        kq, kp = slot // 2, slot % 2
        return member((q + kq) % nq, p if kp == 0 else 1 - p)

    x_in, xc_in, v_in, db_in, da_in = {}, {}, {}, {}, {}

    for kb in range(1, nb):
        xc_in[kb] = send(x_ref, xc.at[kb], xc_s.at[kb], xc_r.at[kb], line(kb))
    for kq in range(1, nq):
        slot = 2 * kq
        x_in[slot] = send(x_ref, xr.at[slot], xr_s.at[slot], xr_r.at[slot], slot_member(slot))
    x_in[1] = send(x_ref, xr.at[1], xr_s.at[1], xr_r.at[1], partner)
    for kq in range(1, nq):
        slot = 2 * kq
        v_in[slot] = send(v_ref, v0.at[slot], v0_s.at[slot], v0_r.at[slot], slot_member(slot))
    v_in[1] = send(v_ref, v0.at[1], v0_s.at[1], v0_r.at[1], partner)
    for kb in range(1, nb):
        db_in[kb] = send(db.at[0], db.at[kb], db_s.at[kb], db_r.at[kb], line(kb))
    for slot in range(1, na):
        da_in[slot] = send(da.at[0], da.at[slot], da_s.at[slot], da_r.at[slot], slot_member(slot))

    def squares(x):
        xf = x.astype(F32)
        sq = xf * xf
        high = sq.astype(BF16)
        return high, (sq - high.astype(F32)).astype(BF16)

    wide = jnp.ones((feats, 128), BF16)
    thin = jnp.ones((8, feats), BF16)

    def dot(l, r, dims):
        return lax.dot_general(l, r, dims, preferred_element_type=F32)

    def store_norm(kb, x):
        high, low = squares(x)
        hj[kb] = sharp * (dot(high, wide, NN) + dot(low, wide, NN))

    def row_norm(x):
        high, low = squares(x)
        return (sharp * (dot(thin, high, NT) + dot(thin, low, NT)))[0:1, :]

    def unit(kb, kq, xj, xi, hi, diagonal=False):
        g = dot(xj, xi, NT)
        hcol = hj[kb]
        for half in range(2):
            lanes = slice(half * span, (half + 1) * span)
            e = jnp.exp2((2.0 * sharp) * g[:, lanes] - (hcol + hi[:, lanes]))
            if diagonal and half == 0:
                rows = lax.broadcasted_iota(jnp.int32, (span, span), 0)
                cols = lax.broadcasted_iota(jnp.int32, (span, span), 1)
                e = jnp.where(rows == cols, 0.0, e)
            at[kb, :, (2 * kq + half) * span:(2 * kq + half + 1) * span] = e.astype(BF16)

    def others(body):
        if nb <= 4:
            for kb in range(1, nb):
                body(kb)
        else:
            def looped(kb, carry):
                body(kb)
                return carry
            lax.fori_loop(1, nb, looped, 0)

    own = x_ref[...]
    store_norm(0, own)
    x_in[1].wait_recv()
    xi = jnp.concatenate([own, xr[1]], axis=0)
    hi0 = row_norm(xi)
    unit(0, 0, own, xi, hi0, diagonal=True)

    def pass_on(slot):
        x_in[slot].wait_recv()
        x_in[slot + 1] = send(
            xr.at[slot], xr.at[slot + 1], xr_s.at[slot + 1], xr_r.at[slot + 1], partner
        )

    def first(kb):
        xj = xc[kb]
        store_norm(kb, xj)
        unit(kb, 0, xj, xi, hi0)

    for kq in range(1, nq):
        pass_on(2 * kq)
    for kq in range(1, nq):
        slot = 2 * kq
        v_in[slot].wait_recv()
        v_in[slot + 1] = send(
            v0.at[slot], v0.at[slot + 1], v0_s.at[slot + 1], v0_r.at[slot + 1], partner
        )
    his, pairs = [hi0], [xi]
    for kq in range(1, nq):
        x_in[2 * kq + 1].wait_recv()
        pairs.append(jnp.concatenate([xr[2 * kq], xr[2 * kq + 1]], axis=0))
        his.append(row_norm(pairs[kq]))
        unit(0, kq, own, pairs[kq], his[kq])

    for kb in range(1, nb):
        xc_in[kb].wait_recv()

    def rest(kb):
        first(kb)
        for kq in range(1, nq):
            unit(kb, kq, xc[kb], pairs[kq], his[kq])

    others(rest)

    for slot in range(1, na):
        if slot % 2:
            v_in[slot].wait_recv()
        da_in[slot].wait_recv()
    for kb in range(1, nb):
        db_in[kb].wait_recv()
    col_degree = [db[kb] for kb in range(nb)]
    row_degree = [da[slot] for slot in range(na)]

    def to_columns(turn, row_vectors):
        wide_rows = jnp.concatenate(row_vectors, axis=1)
        part = [dot(wide_rows, at[kb], NT) for kb in range(nb)]
        for kb in range(nb):
            zb[turn, 0, :, kb * span:(kb + 1) * span] = part[kb]
        arriving = {
            kb: send(
                zb.at[turn, 0], zb.at[turn, kb], zb_s.at[turn, kb], zb_r.at[turn, kb], line(kb)
            )
            for kb in list(range(2, nb)) + [1]
        }
        for step in range(1, nb):
            arriving[step].wait_recv()
            for kb in range(nb):
                there = (kb - step) % nb
                part[kb] = part[kb] + zb[turn, step, :, there * span:(there + 1) * span]
        return [part[kb] / col_degree[kb] for kb in range(nb)]

    def to_rows(col_vectors):
        part = dot(col_vectors[0], at[0], NN)
        for kb in range(1, nb):
            part = part + dot(col_vectors[kb], at[kb], NN)
        ab[0] = part
        arriving = {
            slot: send(ab.at[0], ab.at[slot], ab_s.at[slot], ab_r.at[slot], slot_member(slot))
            for slot in list(range(2, na)) + [1]
        }
        part = [part[:, slot * span:(slot + 1) * span] for slot in range(na)]
        for step in [1] + list(range(2, na)):
            arriving[step].wait_recv()
            for slot in range(na):
                there = (slot // 2 - step // 2) % nq * 2 + (slot % 2 + step % 2) % 2
                part[slot] = part[slot] + ab[step, :, there * span:(there + 1) * span]
        return [part[slot] / row_degree[slot] for slot in range(na)]

    def rounded(vectors):
        return [piece.astype(BF16) for piece in vectors]

    vectors, on_rows, turn = [v0[slot] for slot in range(na)], True, 0
    for it in range(ITERS):
        if on_rows:
            vectors = to_columns(turn, rounded(vectors))
            turn += 1
        else:
            vectors = to_rows(rounded(vectors))
        on_rows = not on_rows
    mine = vectors[0]

    held = jnp.abs(mine)
    for kb in range(1, nb):
        held = held + jnp.abs(vectors[kb])
    sums = jnp.sum(held, axis=1, keepdims=True)
    eye = lax.broadcasted_iota(jnp.int32, (nk, 128), 0) == lax.broadcasted_iota(
        jnp.int32, (nk, 128), 1
    )
    mg[0] = jnp.sum(jnp.where(eye, sums, 0.0), axis=0, keepdims=True)

    mg_in = {
        slot: send(mg.at[0], mg.at[slot], mg_s.at[slot], mg_r.at[slot], slot_member(slot))
        for slot in list(range(2, na)) + [1]
    }
    for copy in pending[:-(na - 1)]:
        copy.wait_send()
    for slot in range(1, na):
        mg_in[slot].wait_recv()
    every = jnp.sum(mg[...], axis=0)
    mean = jnp.sum(jnp.where(eye, every, 0.0), axis=1, keepdims=True) / (span * nd)
    o_ref[...] = mine / (mean + 1e-06)
    for slot in range(1, na):
        mg_in[slot].wait_send()


def solution(mesh):
    nr, nc = mesh.shape["rows"], mesh.shape["cols"]
    low = 1
    while low * nc < nr // low:
        low *= 2
    na, nb = low * nc, nr // low

    def body(points, start_vectors, degree):
        span, feats = points.shape
        nk = start_vectors.shape[0]
        dma = pltpu.SemaphoreType.DMA
        turns = (ITERS + 1) // 2
        return pl.pallas_call(
            functools.partial(kernel, na, nb, nc),
            out_shape=pltpu.VMEM((nk, span), F32),
            in_specs=[pl.BlockSpec(memory_space=pl.ANY)] * 3,
            out_specs=pl.BlockSpec(memory_space=pltpu.VMEM),
            scratch_shapes=[
                pltpu.VMEM((na, span, feats), BF16),
                pltpu.VMEM((nb, span, feats), BF16),
                pltpu.VMEM((na, nk, span), F32),
                pltpu.VMEM((nb, 1, span), F32),
                pltpu.VMEM((na, 1, span), F32),
                pltpu.VMEM((turns, nb, nk, nb * span), F32),
                pltpu.VMEM((na, nk, na * span), F32),
                pltpu.VMEM((na, 1, 128), F32),
                pltpu.VMEM((nb, span, na * span), BF16),
                pltpu.VMEM((nb, span, 128), F32),
                pltpu.VMEM((1, span), BF16),
                dma((3,)),
                dma((na,)), dma((na,)), dma((nb,)), dma((nb,)), dma((na,)), dma((na,)),
                dma((nb,)), dma((nb,)), dma((na,)), dma((na,)),
                dma((turns, nb)), dma((turns, nb)), dma((na,)), dma((na,)),
                dma((na,)), dma((na,)),
            ],
            compiler_params=pltpu.CompilerParams(collective_id=0, has_side_effects=True),
        )(points, start_vectors, degree.reshape(1, span))

    return jax.shard_map(
        body,
        mesh=mesh,
        in_specs=(P(("rows", "cols"), None), P(None, ("rows", "cols")), P(("rows", "cols"))),
        out_specs=P(None, ("rows", "cols")),
        check_vma=False,
    )
```
